32 devices in a mesh: gx: 4 (over y, x), gy: 2 (over core), gz: 4 (over z).
Axes of the slice: x: 2, y: 2, z: 4, core: 2. Of those that a mesh axis runs over, the one named last changes fastest.
Arguments:
- start_block: float32 [64, 3, 8, 16, 512], P(None, None, 'gx', 'gy', 'gz'), may hold values from -6 to 6
- stiff_field: float32 [8, 16, 512], P('gx', 'gy', 'gz'), may hold values from 0.5 to 2
- shift_field: float32 [8, 16, 512], P('gx', 'gy', 'gz'), may hold values from 0.25 to 2
- mass_field: float32 [8, 16, 512], P('gx', 'gy', 'gz'), may hold values from 0.5 to 2
Outputs:
- modes: float32 [64, 3, 8, 16, 512], P(None, None, 'gx', 'gy', 'gz')
- ritz: float32 [64, 64], replicated
The draws below stay inside these ranges and needn't reach their ends.
All inputs are finite; a program needn't handle non-finite values. Where the reference program divides by a largest or mean magnitude, that divisor is 1e-20 or more.
Results may differ from the reference program's by a relative error of at most 0.0003.
Values sent between devices are 32-bit elements; how exact they have to be, the bound alone decides.
A program may use at most 128 MiB of HBM per device.

```python
import math
import jax
import jax.numpy as jnp
from jax import lax

MODES = 64
ITERS = 2
FILTER = 4
NX = 8
NY = 16
NZ = 512
DOFS = 196608


def steps_of(rng, shape, cuts, smallest, top_value):
    def one(axis_at, parts):
        steps = jax.random.uniform(jax.random.fold_in(jax.random.fold_in(rng, 6), axis_at), (parts,), jnp.float32, smallest / len(cuts), top_value / len(cuts))
        return jnp.repeat(jnp.exp(steps), shape[axis_at] // parts).reshape((-1,) + (1,) * (len(shape) - axis_at - 1))

    gain = one(*cuts[0])
    for cut in cuts[1:]:
        gain = gain * one(*cut)
    return gain


def noise(key, shape, scale, limit, cuts=(), dtype=jnp.bfloat16):
    result = jax.random.normal(key, shape, jnp.float32) * scale
    if len(cuts) > 0:
        result = steps_of(key, shape, cuts, -0.22, 0.18) * result
    return jnp.clip(result, min=-limit, max=limit).astype(dtype)


def setup_inputs(seed: int = 0) -> dict:
    seeds = jax.random.split(jax.random.key(seed), 5)
    start_block = noise(seeds[0], (MODES, 3, NX, NY, NZ), 1.0, 6.0, ((2, 4), (3, 2), (4, 4)), jnp.float32)
    stiff_field = jnp.clip(jnp.exp(math.log(2.0) - 1.3862944 * jax.random.uniform(seeds[1], (NX, NY, NZ), jnp.float32) ** steps_of(seeds[1], (NX, NY, NZ), ((0, 4), (1, 2), (2, 4)), -0.2, 0.2)), 0.5, 2.0)
    shift_field = jnp.clip(jnp.exp(math.log(2.0) - 2.0794415 * jax.random.uniform(seeds[2], (NX, NY, NZ), jnp.float32) ** steps_of(seeds[2], (NX, NY, NZ), ((0, 4), (1, 2), (2, 4)), -0.2, 0.2)), 0.25, 2.0)
    mass_field = jnp.clip(jnp.exp(math.log(2.0) - 1.3862944 * jax.random.uniform(seeds[3], (NX, NY, NZ), jnp.float32) ** steps_of(seeds[3], (NX, NY, NZ), ((0, 4), (1, 2), (2, 4)), -0.2, 0.2)), 0.5, 2.0)
    return {"start_block": start_block, "stiff_field": stiff_field, "shift_field": shift_field, "mass_field": mass_field}


def lower_solve(lower_mat, rhs):
    return lax.linalg.triangular_solve(lower_mat, rhs, left_side=True, lower=True)

def lower_trans_solve(lower_mat, rhs):
    return lax.linalg.triangular_solve(lower_mat, rhs, left_side=True, lower=True, transpose_a=True)

def hidot(left, right):
    return jnp.dot(left.astype(jnp.float32), right.astype(jnp.float32), precision=lax.Precision.HIGHEST, preferred_element_type=jnp.float32)

def gram_of(left, right):
    return hidot(left.reshape(left.shape[0], -1), right.reshape(right.shape[0], -1).T)

def combine(coeffs, vectors):
    flat = hidot(coeffs.T, vectors.reshape(vectors.shape[0], -1))
    return flat.reshape((coeffs.shape[1],) + vectors.shape[1:])

def stiffness(field, stiff_field, shift_field):
    scaled = stiff_field * field
    padded = jnp.pad(scaled, ((0, 0), (0, 0), (1, 1), (1, 1), (1, 1)))
    beside_all = padded[:, :, 2:, 1:-1, 1:-1] + padded[:, :, :-2, 1:-1, 1:-1]
    beside_all = beside_all + padded[:, :, 1:-1, 2:, 1:-1] + padded[:, :, 1:-1, :-2, 1:-1]
    beside_all = beside_all + padded[:, :, 1:-1, 1:-1, 2:] + padded[:, :, 1:-1, 1:-1, :-2]
    laplace = 6.0 * scaled - beside_all
    summed = jnp.sum(field, axis=1, keepdims=True)
    return stiff_field * laplace + shift_field * (field + 0.5 * summed)

def ritz_filter(pencil_k, pencil_m, mode_count):
    factor = jnp.linalg.cholesky(pencil_m)
    partial_value = lower_solve(factor, pencil_k)
    reduced = lower_solve(factor, partial_value.T).T
    gershgorin = jnp.max(jnp.sum(jnp.abs(reduced), axis=1))
    search = factor.T[:, :mode_count]
    for sweep_index in range(FILTER):
        search = search - hidot(reduced, search) / gershgorin
    correlation = hidot(search.T, search)
    small_factor = jnp.linalg.cholesky(correlation)
    orthonormal = lower_solve(small_factor, search.T).T
    coeffs = lower_trans_solve(factor, orthonormal)
    ritz_matrix = hidot(orthonormal.T, hidot(reduced, orthonormal))
    return (coeffs, ritz_matrix)

def reference(start_block, stiff_field, shift_field, mass_field):
    count = MODES
    start_image = stiffness(start_block, stiff_field, shift_field)
    mass_gram = gram_of(start_block, mass_field * start_block) / DOFS
    stiff_gram = gram_of(start_block, start_image) / DOFS
    factor = jnp.linalg.cholesky(mass_gram)
    current = lower_solve(factor, start_block.reshape(count, -1)).reshape(start_block.shape)
    stiff_image = lower_solve(factor, start_image.reshape(count, -1)).reshape(start_block.shape)
    ritz_matrix = lower_solve(factor, lower_solve(factor, stiff_gram).T).T
    diagonal = 6.0 * stiff_field * stiff_field + 1.5 * shift_field
    previous = None
    for iteration in range(ITERS):
        residual = (stiff_image - mass_field * combine(ritz_matrix, current)) / diagonal
        stiff_resid = stiffness(residual, stiff_field, shift_field)
        if iteration == 0:
            search_set = jnp.concatenate([current, residual], axis=0)
            image_set = jnp.concatenate([stiff_image, stiff_resid], axis=0)
        else:
            search_set = jnp.concatenate([current, residual, previous[0]], axis=0)
            image_set = jnp.concatenate([stiff_image, stiff_resid, previous[1]], axis=0)
        pencil_k = gram_of(search_set, image_set) / DOFS
        pencil_m = gram_of(search_set, mass_field * search_set) / DOFS
        coeffs, ritz_matrix = ritz_filter(pencil_k, pencil_m, count)
        current = combine(coeffs, search_set)
        stiff_image = combine(coeffs, image_set)
        previous = (combine(coeffs[count:], search_set[count:]), combine(coeffs[count:], image_set[count:]))
    return (current, ritz_matrix)
```

```python
import functools

import jax
import jax.numpy as jnp
from jax import lax
from jax.experimental import pallas as pl
from jax.experimental.pallas import tpu as pltpu
from jax.sharding import PartitionSpec as P

ITERS = 2
FILTER = 4
AXES = ("gx", "gy", "gz")
SMALL = lax.Precision.HIGHEST
BIG = lax.Precision.HIGHEST
PANEL = 8


def mm(a, b, precision=SMALL):
    return lax.dot_general(a, b, (((1,), (0,)), ((), ())), precision=precision, preferred_element_type=jnp.float32)


def mt(a, b, precision=SMALL):
    return lax.dot_general(a, b, (((1,), (1,)), ((), ())), precision=precision, preferred_element_type=jnp.float32)


def lower_inverse(matrix):
    n = matrix.shape[0]
    rows = lax.broadcasted_iota(jnp.int32, (n, n), 0)
    cols = lax.broadcasted_iota(jnp.int32, (n, n), 1)
    aug = jnp.concatenate([matrix, jnp.where(rows == cols, 1.0, 0.0)], axis=1)
    width = 2 * n
    done = []
    for start in range(0, n, PANEL):
        left = [jnp.broadcast_to(aug[:, start + m : start + m + 1], aug.shape) for m in range(PANEL)]
        head = [aug[m : m + 1, :] for m in range(PANEL)]
        rest = aug[PANEL:, :]
        for m in range(PANEL):
            pivot = left[m][m : m + 1, :]
            inverse = 1.0 / pivot
            scaled = head[m] * inverse
            for k in range(m + 1, PANEL):
                factor = left[m][k : k + 1, :]
                head[k] = head[k] - factor * scaled
                left[k] = left[k] - left[m] * (factor * inverse)
            if rest.shape[0] > 0:
                rest = rest - left[m][PANEL:, :] * scaled
            done.append(head[m] * lax.rsqrt(pivot))
        aug = rest
    full = jnp.concatenate(done, axis=0)
    return full[:, n:width]


def filtered(ga, columns, count):
    linv = jnp.concatenate(columns, axis=1)
    h = mt(mm(linv, ga), linv)
    total = h.shape[0]
    inv_c = 1.0 / jnp.max(jnp.sum(jnp.abs(h), axis=1, keepdims=True), axis=0, keepdims=True)
    rows = lax.broadcasted_iota(jnp.int32, (count, total), 0)
    cols = lax.broadcasted_iota(jnp.int32, (count, total), 1)
    search_t = jnp.where(rows == cols, 1.0, 0.0)
    for _ in range(FILTER):
        search_t = search_t - mt(search_t, h) * inv_c
    small = lower_inverse(mt(search_t, search_t))
    ortho_t = mm(small, search_t)
    coeffs_t = mm(ortho_t, linv)
    of_resid = mm(ortho_t, columns[1])
    half = mm(ortho_t, h)
    return coeffs_t, of_resid, mt(half, ortho_t), mt(ortho_t, half)


def emit_faces(v_ref, g_ref, faces, x_count, y_count):
    xlo, xhi, ylo, yhi, zlo, zhi = faces
    comps = v_ref.shape[0]
    lanes = v_ref.shape[-1]
    lane = lax.broadcasted_iota(jnp.int32, zlo.shape, 1)
    zlo[...] = jnp.zeros_like(zlo)
    zhi[...] = jnp.zeros_like(zhi)

    def body(i, _):
        x, y = i // y_count, i % y_count
        g = g_ref[x, y]
        for c in range(comps):
            h = g * v_ref[c, x, y]
            r = c * x_count * y_count + i
            zlo[...] = jnp.where(lane == r, pltpu.roll(h, r, 1), zlo[...])
            zhi[...] = jnp.where(lane == r, pltpu.roll(h, r + 1, 1), zhi[...])
        return 0

    lax.fori_loop(0, x_count * y_count, body, 0)

    def x_faces(y, _):
        for c in range(comps):
            xlo[c, y] = g_ref[0, y] * v_ref[c, 0, y]
            xhi[c, y] = g_ref[x_count - 1, y] * v_ref[c, x_count - 1, y]
        return 0

    lax.fori_loop(0, y_count, x_faces, 0)
    for x in range(x_count):
        for c in range(comps):
            ylo[c, x] = g_ref[x, 0] * v_ref[c, x, 0]
            yhi[c, x] = g_ref[x, y_count - 1] * v_ref[c, x, y_count - 1]


def joined(ref, x, y):
    return jnp.concatenate([ref[c, x, y] for c in range(ref.shape[0])], axis=1)


def store(ref, x, y, value):
    lanes = ref.shape[-1]
    for c in range(ref.shape[0]):
        ref[c, x, y] = value[:, c * lanes : (c + 1) * lanes]


def wide(row, comps):
    return jnp.concatenate([row] * comps, axis=1)


def prepare_kernel(s_ref, g_ref, v_ref, *faces):
    comps, x_count, y_count, count, lanes = v_ref.shape
    for c in range(comps):
        for x in range(x_count):
            for y in range(y_count):
                v_ref[c, x, y] = s_ref[:, c, x, y, :]
    emit_faces(v_ref, g_ref, faces, x_count, y_count)


def stiff_kernel(v_ref, xm, xp, ym, yp, zm, zp, g_ref, e_ref, rho_ref, *rest):
    *others, kv_ref, sums_ref, pad = rest
    comps, x_count, y_count, count, lanes = v_ref.shape
    lane = lax.broadcasted_iota(jnp.int32, (count, lanes), 1)
    for c in range(comps):
        for x in range(x_count):
            pad[c, x + 1, 0] = ym[c, x]
            pad[c, x + 1, y_count + 1] = yp[c, x]

    def fill(y, _):
        for c in range(comps):
            pad[c, 0, y + 1] = xm[c, y]
            pad[c, x_count + 1, y + 1] = xp[c, y]
            for x in range(x_count):
                pad[c, x + 1, y + 1] = g_ref[x, y] * v_ref[c, x, y]
        return 0

    lax.fori_loop(0, y_count, fill, 0)
    sums_ref[...] = jnp.zeros_like(sums_ref)

    def body(i, _):
        x, y = i // y_count, i % y_count
        g, e, rho = g_ref[x, y], e_ref[x, y], rho_ref[x, y]
        v = [v_ref[c, x, y] for c in range(comps)]
        summed = v[0]
        for c in range(1, comps):
            summed = summed + v[c]
        images = []
        for c in range(comps):
            r = c * x_count * y_count + i
            h = pad[c, x + 1, y + 1]
            beside = pad[c, x + 2, y + 1] + pad[c, x, y + 1]
            beside = beside + pad[c, x + 1, y + 2] + pad[c, x + 1, y]
            before = jnp.where(lane == 0, pltpu.roll(zm[...], lanes - r, 1), pltpu.roll(h, 1, 1))
            after = jnp.where(lane == lanes - 1, pltpu.roll(zp[...], lanes - 1 - r, 1), pltpu.roll(h, lanes - 1, 1))
            image = g * (6.0 * h - (beside + before + after)) + e * (v[c] + 0.5 * summed)
            kv_ref[c, x, y] = image
            images.append(image)
        here = jnp.concatenate(v, axis=1)
        right = jnp.concatenate([here * wide(rho, comps), jnp.concatenate(images, axis=1)], axis=0)
        left = jnp.concatenate([here] + [joined(o, x, y) for o in others], axis=0)
        sums_ref[...] += mt(left, right, BIG)
        return 0

    lax.fori_loop(0, x_count * y_count, body, 0)


def start_kernel(dof_count, sums_ref, s_ref, ks_ref, g_ref, e_ref, rho_ref, x_ref, kx_ref, r_ref, theta_ref, *faces):
    comps, x_count, y_count, count, lanes = s_ref.shape
    scale = 1.0 / dof_count
    mass = sums_ref[:, :count] * scale
    stiff = sums_ref[:, count:] * scale
    linv = lower_inverse(mass)
    half = mm(linv, stiff)
    theta = mt(half, linv)
    theta_ref[...] = theta
    stacked = jnp.concatenate([linv, mm(mt(linv, half), linv)], axis=0)

    def body(i, _):
        x, y = i // y_count, i % y_count
        g, e, rho = g_ref[x, y], e_ref[x, y], rho_ref[x, y]
        diag = 6.0 * g * g + 1.5 * e
        both = mm(stacked, joined(s_ref, x, y), BIG)
        image = mm(linv, joined(ks_ref, x, y), BIG)
        store(x_ref, x, y, both[:count])
        store(kx_ref, x, y, image)
        store(r_ref, x, y, (image - wide(rho, comps) * both[count:]) * wide(1.0 / diag, comps))
        return 0

    lax.fori_loop(0, x_count * y_count, body, 0)
    emit_faces(r_ref, g_ref, faces, x_count, y_count)


def first_kernel(dof_count, sums_ref, theta_ref, x_ref, kx_ref, r_ref, kr_ref, g_ref, e_ref, rho_ref,
                 x1_ref, kx1_ref, p_ref, kp_ref, r1_ref, theta1_ref, grams_ref, *rest):
    faces = rest
    comps, x_count, y_count, count, lanes = x_ref.shape
    n = count
    scale = 1.0 / dof_count
    sums = sums_ref[...] * scale
    mrr, arr = sums[:n, :n], sums[:n, n:]
    mxr, axr = sums[n:, :n], sums[n:, n:]
    turned = sums.T
    mrx, arx = turned[:n, n:], turned[n:, n:]
    tr = lower_inverse(mrr - mt(mrx, mrx))
    eye = jnp.where(lax.broadcasted_iota(jnp.int32, (n, n), 0) == lax.broadcasted_iota(jnp.int32, (n, n), 1), 1.0, 0.0)
    zero = jnp.zeros((n, n), jnp.float32)
    columns = [jnp.concatenate([eye, -mm(tr, mrx)], axis=0), jnp.concatenate([zero, tr], axis=0)]
    ga = jnp.concatenate([jnp.concatenate([theta_ref[...], axr], axis=1), jnp.concatenate([arx, arr], axis=1)], axis=0)
    coeffs_t, cr, theta, theta_t = filtered(ga, columns, n)
    theta1_ref[...] = theta
    mpp = mt(mm(cr, mrr), cr)
    app = mt(mm(cr, arr), cr)
    grams_ref[0] = mt(cr, mm(coeffs_t, jnp.concatenate([mxr, mrr], axis=0)))
    grams_ref[1] = mpp
    half = mm(coeffs_t, jnp.concatenate([axr, arr], axis=0))
    grams_ref[2] = mt(half, cr)
    grams_ref[3] = app
    grams_ref[4] = mt(cr, half)
    stacked = jnp.concatenate([coeffs_t, mm(theta_t, coeffs_t)], axis=0)

    def body(i, _):
        x, y = i // y_count, i % y_count
        g, e, rho = g_ref[x, y], e_ref[x, y], rho_ref[x, y]
        diag = 6.0 * g * g + 1.5 * e
        resid = joined(r_ref, x, y)
        image_r = joined(kr_ref, x, y)
        both = mm(stacked, jnp.concatenate([joined(x_ref, x, y), resid], axis=0), BIG)
        image = mm(coeffs_t, jnp.concatenate([joined(kx_ref, x, y), image_r], axis=0), BIG)
        store(x1_ref, x, y, both[:n])
        store(p_ref, x, y, mm(cr, resid, BIG))
        store(kx1_ref, x, y, image)
        store(kp_ref, x, y, mm(cr, image_r, BIG))
        store(r1_ref, x, y, (image - wide(rho, comps) * both[n:]) * wide(1.0 / diag, comps))
        return 0

    lax.fori_loop(0, x_count * y_count, body, 0)
    emit_faces(r1_ref, g_ref, faces, x_count, y_count)


def last_kernel(dof_count, sums_ref, theta_ref, grams_ref, x_ref, r_ref, p_ref, out_ref, ritz_ref):
    comps, x_count, y_count, count, lanes = x_ref.shape
    n = count
    sums = sums_ref[...] * (1.0 / dof_count)
    mrr, arr = sums[:n, :n], sums[:n, n:]
    mxr, axr = sums[n : 2 * n, :n], sums[n : 2 * n, n:]
    mpr, apr = sums[2 * n :, :n], sums[2 * n :, n:]
    bp, mpp, axp, app, apx = (grams_ref[k] for k in range(5))
    turned = sums.T
    br, arx, arp = turned[:n, n : 2 * n], turned[n:, n : 2 * n], turned[n:, 2 * n :]
    tr = lower_inverse(mrr - mt(br, br))
    lpr = mt(mpr - mt(bp, br), tr)
    tp = lower_inverse(mpp - mt(bp, bp) - mt(lpr, lpr))
    rx = -mm(tr, br)
    px = -mm(tp, bp + mm(lpr, rx))
    pr = -mm(tp, mm(lpr, tr))
    eye = jnp.where(lax.broadcasted_iota(jnp.int32, (n, n), 0) == lax.broadcasted_iota(jnp.int32, (n, n), 1), 1.0, 0.0)
    zero = jnp.zeros((n, n), jnp.float32)

    def block(rows):
        return jnp.concatenate([jnp.concatenate(row, axis=1) for row in rows], axis=0)

    columns = [jnp.concatenate(blocks, axis=0) for blocks in ((eye, rx, px), (zero, tr, pr), (zero, zero, tp))]
    ga = block([[theta_ref[...], axr, axp], [arx, arr, arp], [apx, apr, app]])
    coeffs_t, _, theta, _ = filtered(ga, columns, n)
    ritz_ref[...] = theta
    for x in range(x_count):
        for y in range(y_count):
            value = mm(coeffs_t, jnp.concatenate([joined(v, x, y) for v in (x_ref, r_ref, p_ref)], axis=0), BIG)
            for c in range(comps):
                out_ref[:, c, x, y, :] = value[:, c * lanes : (c + 1) * lanes]


def call(kernel, out_shapes, scratch, *args):
    spec = pl.BlockSpec(memory_space=pltpu.VMEM)
    return pl.pallas_call(
        kernel,
        out_shape=[jax.ShapeDtypeStruct(s, jnp.float32) for s in out_shapes],
        in_specs=[spec] * len(args),
        out_specs=[spec] * len(out_shapes),
        scratch_shapes=[pltpu.VMEM(s, jnp.float32) for s in scratch],
        compiler_params=pltpu.CompilerParams(vmem_limit_bytes=60000 * 1024),
    )(*args)


def exchange(faces):
    xlo, xhi, ylo, yhi, zlo, zhi = faces
    received = []
    for axis, low, high in zip(AXES, (xlo, ylo, zlo), (xhi, yhi, zhi)):
        devices = lax.axis_size(axis)
        up = [(i, i + 1) for i in range(devices - 1)]
        down = [(j, i) for i, j in up]
        received += [lax.ppermute(high, axis, up), lax.ppermute(low, axis, down)]
    return received


def reduced(sums):
    return lax.psum(sums, AXES)


def local(start_block, stiff_field, shift_field, mass_field):
    count, comps, x_count, y_count, lanes = start_block.shape
    devices = lax.axis_size("gx") * lax.axis_size("gy") * lax.axis_size("gz")
    dof_count = float(comps * stiff_field.size * devices)
    assert comps * x_count * y_count <= lanes
    g, e, rho = (f[:, :, None, :] for f in (stiff_field, shift_field, mass_field))
    field = (comps, x_count, y_count, count, lanes)
    small = (count, count)
    face_shapes = [(comps, y_count, count, lanes)] * 2 + [(comps, x_count, count, lanes)] * 2 + [(count, lanes)] * 2
    padded = (comps, x_count + 2, y_count + 2, count, lanes)

    def stiff(v, faces, *others):
        shapes = [field, ((1 + len(others)) * count, 2 * count)]
        return call(stiff_kernel, shapes, [padded], v, *exchange(faces), g, e, rho, *others)

    s, *faces = call(prepare_kernel, [field] + face_shapes, [], start_block, g)
    ks, sums = stiff(s, faces)
    x, kx, r, theta, *faces = call(
        functools.partial(start_kernel, dof_count), [field] * 3 + [small] + face_shapes, [], reduced(sums), s, ks, g, e, rho
    )
    kr, sums = stiff(r, faces, x)
    x1, kx1, p, kp, r1, theta, grams, *faces = call(
        functools.partial(first_kernel, dof_count),
        [field] * 5 + [small, (5,) + small] + face_shapes,
        [],
        reduced(sums), theta, x, kx, r, kr, g, e, rho,
    )
    _, sums = stiff(r1, faces, x1, p)
    modes, ritz = call(
        functools.partial(last_kernel, dof_count), [start_block.shape, small], [], reduced(sums), theta, grams, x1, r1, p
    )
    return modes, ritz


def solution(mesh):
    block = P(None, None, *AXES)
    node = P(*AXES)
    return jax.shard_map(local, mesh=mesh, in_specs=(block, node, node, node), out_specs=(block, P()), check_vma=False)
```
